32 devices in a mesh: dp: 8 (over y, x, core), mp: 4 (over z).
Axes of the slice: x: 2, y: 2, z: 4, core: 2. Of those that a mesh axis runs over, the one named last changes fastest.
Arguments:
- hidden: bfloat16 [4096, 16384], P('dp', 'mp'), may hold values from -64 to 64
- key_weight: bfloat16 [16384, 1024], P(('mp', 'dp')), may hold values from -0.046875 to 0.046875
- key_state: float32 [16384], P(('mp', 'dp')), may hold values from 2.9802323e-09 to 1.1920929e-07
- key_cotangent: bfloat16 [4096, 1024], P('dp'), may hold values from -6 to 6
- doc_lengths: int32 [16, 4], P('dp'), may hold values from 1 to 128, 256 in all within a row
Outputs:
- input_grad: bfloat16 [4096, 16384], P('dp', 'mp')
- new_weight: bfloat16 [16384, 1024], P(('mp', 'dp'))
- new_state: float32 [16384], P(('mp', 'dp'))
The draws below stay inside these ranges and needn't reach their ends.
Inputs may be any that keep to these rules, and one draw needn't show every extreme that they name: `doc_lengths`: each row lists the lengths of the documents of one sequence, in order, summing to 256.
All inputs are finite; a program needn't handle non-finite values.
Results may differ from the reference program's by a relative error of at most 0.0045.
Values may be sent and summed in bfloat16 or wider, within the bound.
A program may use at most 128 MiB of HBM per device.

```python
import math
import jax
import jax.numpy as jnp
import numpy as np
from jax import lax

D = 16384
HD = 128
LEN = 256
DOCS = 4
KVW = 1024
MOST = 128
TOK_DEV = 512
SEQS = 16
TOKENS = 4096
ROWS_DEV = 512


def draw_hidden(key, part):
    draw_keys = jax.random.split(key, 5)
    base_draw = jax.random.normal(draw_keys[0], (TOKENS, D), jnp.float32)
    rising = 1.0 + 2.0 * jnp.arange(D, dtype=jnp.float32) / (D - 1)
    col_scale = jnp.exp(jax.random.uniform(draw_keys[1], (D,), jnp.float32, math.log(0.5), math.log(2.0)))
    row_scale = jnp.exp(jax.random.uniform(draw_keys[2], (TOKENS, 1), jnp.float32, math.log(0.5), math.log(2.0)))
    targets = jax.random.randint(draw_keys[4], (TOKENS // TOK_DEV,), 0, D // ROWS_DEV)
    token_block = jnp.arange(TOKENS) // TOK_DEV
    feature_block = jnp.arange(D) // ROWS_DEV
    amplified = 1.0 + 3.0 * (targets[token_block][:, None] == feature_block[None, :]).astype(jnp.float32)
    spiked = base_draw * row_scale * (col_scale * rising)[None, :] * amplified
    return jnp.clip(spiked, -64.0, 64.0).astype(jnp.bfloat16)


def level_of(stream_key, dims, shards, smallest, high):
    def one(axis_at, parts):
        steps = jax.random.uniform(jax.random.fold_in(jax.random.fold_in(stream_key, 6), axis_at), (parts,), jnp.float32, smallest / len(shards), high / len(shards))
        return jnp.repeat(jnp.exp(steps), dims[axis_at] // parts).reshape((-1,) + (1,) * (len(dims) - axis_at - 1))

    factor_of = one(*shards[0])
    for cut in shards[1:]:
        factor_of = factor_of * one(*cut)
    return factor_of


def split_up(count, total, bound, slope):
    portions = [(1 << 20) // math.isqrt(rank ** slope) + 1 for rank in range(2, count + 1)]
    rest, holding = total - bound - (count - 1), [1] * (count - 1)
    while rest > 0:
        free = [i for i in range(count - 1) if holding[i] < bound]
        pool, remaining = sum([portions[i] for i in free]), rest
        for i in free:
            addition = min(bound - holding[i], max(1, remaining * portions[i] // pool), rest)
            holding[i] = holding[i] + addition
            rest = rest - addition
    return np.array([bound] + holding)


def uneven(rng, number_of, total, bound, skew):
    if number_of == 2:
        one = jax.random.randint(rng, (), max(1, total - bound), min(bound, total - 1) + 1)
        return jnp.stack([one, total - one])
    tallies = jnp.asarray(split_up(number_of, total, bound, skew), jnp.int32)
    twos = (number_of - 1) // 2
    donor, sink = tallies[1:1 + 2 * twos:2], tallies[2:2 + 2 * twos:2]
    room = jnp.minimum(donor - 1, bound - sink)
    shifted = jax.random.randint(jax.random.fold_in(rng, 1), (twos,), 0, 1 << 20) % (room + 1)
    tallies = tallies.at[1:1 + 2 * twos:2].set(donor - shifted).at[2:2 + 2 * twos:2].set(sink + shifted)
    return tallies[jax.random.permutation(jax.random.fold_in(rng, 2), number_of)]


def normal_values(stream_key, shape, scale, reach, pieces=(), held_as=jnp.bfloat16):
    gain = level_of(stream_key, shape, pieces, -0.22, 0.18) if pieces else 1.0
    values = jax.random.normal(stream_key, shape, jnp.float32) * scale * gain
    return jnp.minimum(jnp.maximum(values, -reach), reach).astype(held_as)


def setup_inputs(seed: int = 0) -> dict:
    streams_of = jax.random.split(jax.random.key(seed), 6)
    return {
        "hidden": draw_hidden(jax.random.fold_in(streams_of[5], 71), 0),
        "key_weight": normal_values(streams_of[1], (D, KVW), D ** -0.5, 0.046875, ((0, 32),)),
        "key_state": jnp.clip(jnp.exp(math.log(1.1920928955078125e-07) - 3.6888794 * jax.random.uniform(streams_of[2], (D,), jnp.float32) ** level_of(streams_of[2], (D,), ((0, 32),), -0.2, 0.2)), 2.9802322831784522e-09, 1.1920928955078125e-07),
        "key_cotangent": normal_values(streams_of[3], (TOKENS, KVW), 1.0, 6.0, ((0, 8),)),
        "doc_lengths": jax.vmap(lambda own: uneven(own, DOCS, LEN, MOST, 1))(jax.random.split(streams_of[4], SEQS)).reshape((SEQS, DOCS)).astype(jnp.int32),
    }


learn_rate = 0.01

def positions_of(doc_lengths):
    doc_ends = jnp.cumsum(doc_lengths, axis=1).astype(jnp.int32)
    doc_starts = (doc_ends - doc_lengths).astype(jnp.int32)
    places = jnp.arange(LEN, dtype=jnp.int32)
    before = doc_starts[:, None, :] <= places[None, :, None]
    doc_start = lax.optimization_barrier(jnp.max(jnp.where(before, doc_starts[:, None, :], 0), axis=2)).astype(jnp.int32)
    return (places[None, :] - doc_start).reshape(-1).astype(jnp.int32)

def rope_back(cotangent, positions):
    half_dim = HD // 2
    frequency = jnp.exp(-(2.0 * jnp.arange(half_dim, dtype=jnp.float32) / HD) * jnp.log(jnp.float32(500000.0)))
    angles = positions.astype(jnp.float32)[:, None] * frequency[None, :]
    cos_part = jnp.cos(angles)[:, None, :]
    sin_part = jnp.sin(angles)[:, None, :]
    gradients = cotangent.astype(jnp.float32).reshape(cotangent.shape[0], -1, HD)
    first_half = gradients[..., :half_dim]
    second_half = gradients[..., half_dim:]
    rotated = jnp.concatenate([first_half * cos_part + second_half * sin_part, second_half * cos_part - first_half * sin_part], axis=-1)
    return rotated.reshape(cotangent.shape[0], -1).astype(jnp.bfloat16)

def reference(hidden, key_weight, key_state, key_cotangent, doc_lengths):
    positions = positions_of(doc_lengths)
    key_grad = rope_back(key_cotangent, positions)
    weight_grad = lax.dot_general(hidden, key_grad, (((0,), (0,)), ((), ())), preferred_element_type=jnp.float32)
    input_grad = lax.dot_general(key_grad, key_weight, (((1,), (1,)), ((), ())), preferred_element_type=jnp.float32).astype(jnp.bfloat16)
    squared = weight_grad * weight_grad
    squares_sum = jnp.sum(squared)
    clip_factor = jnp.minimum(jnp.float32(1.0), 1.0 / jnp.sqrt(squares_sum + 1e-06))
    row_mean = lax.optimization_barrier(jnp.mean(squared, axis=1))
    new_state = key_state + clip_factor * clip_factor * row_mean
    step_size = learn_rate * clip_factor * weight_grad / (jnp.sqrt(new_state)[:, None] + 1e-10)
    new_weight = (key_weight.astype(jnp.float32) - step_size).astype(jnp.bfloat16)
    return (input_grad, new_weight, new_state)
```

```python
import functools

import jax
import jax.numpy as jnp
from jax import lax
from jax.experimental import pallas as pl
from jax.experimental.pallas import tpu as pltpu
from jax.sharding import PartitionSpec as P

HD = 128
LEN = 256


learn_rate = 0.01


def positions_of(doc_lengths):
    doc_ends = jnp.cumsum(doc_lengths, axis=1)
    doc_starts = doc_ends - doc_lengths
    places = jnp.arange(LEN, dtype=jnp.int32)
    before = doc_starts[:, None, :] <= places[None, :, None]
    doc_start = jnp.max(jnp.where(before, doc_starts[:, None, :], 0), axis=2)
    return (places[None, :] - doc_start).reshape(-1)


def rope_back(cotangent, positions):
    half_dim = HD // 2
    frequency = jnp.exp(
        -(2.0 * jnp.arange(half_dim, dtype=jnp.float32) / HD) * jnp.log(jnp.float32(500000.0))
    )
    angles = positions.astype(jnp.float32)[:, None] * frequency[None, :]
    cos_part = jnp.cos(angles)[:, None, :]
    sin_part = jnp.sin(angles)[:, None, :]
    gradients = cotangent.astype(jnp.float32).reshape(cotangent.shape[0], -1, HD)
    first_half = gradients[..., :half_dim]
    second_half = gradients[..., half_dim:]
    rotated = jnp.concatenate(
        [
            first_half * cos_part + second_half * sin_part,
            second_half * cos_part - first_half * sin_part,
        ],
        axis=-1,
    )
    return rotated.reshape(cotangent.shape[0], -1).astype(jnp.bfloat16)


def update(owned, key_weight, key_state):
    squared = owned * owned
    squares_sum = lax.psum(jnp.sum(squared), ("dp", "mp"))
    clip_factor = jnp.minimum(jnp.float32(1.0), 1.0 / jnp.sqrt(squares_sum + 1e-06))
    row_mean = jnp.mean(squared, axis=1)
    new_state = key_state + clip_factor * clip_factor * row_mean
    step_size = learn_rate * clip_factor * owned / (jnp.sqrt(new_state)[:, None] + 1e-10)
    new_weight = (key_weight.astype(jnp.float32) - step_size).astype(jnp.bfloat16)
    return new_weight, new_state


def shards(hidden, key_weight, key_state, key_cotangent, doc_lengths):
    positions = positions_of(doc_lengths)
    key_grad = rope_back(key_cotangent, positions)
    gathered = lax.dot_general(
        key_grad,
        lax.all_gather(key_weight, "dp", axis=0, tiled=True),
        (((1,), (1,)), ((), ())),
        preferred_element_type=jnp.float32,
    )
    input_grad = gathered.astype(jnp.bfloat16)
    owned = lax.psum_scatter(
        lax.dot_general(
            hidden, key_grad, (((0,), (0,)), ((), ())), preferred_element_type=jnp.float32
        ),
        "dp",
        scatter_dimension=0,
        tiled=True,
    )
    return (input_grad, *update(owned, key_weight, key_state))


COPIES = 64
LOCALS = 9


def exchange(zs, hid, w, state, cot, docs, freq, ig, new_w, new_state, wv, states, cots, lengths, freqs, hh, kga, part, s1x, s1y, r1x, r1y, s2x, s2y, r2x, r2y, wall, g, squares, square_rows, sums, got, local, send, recv, sum_send, sum_recv):
    f32, bf16 = jnp.float32, jnp.bfloat16
    rows, kvw = wv.shape
    tokens = cots.shape[0]
    half, step, cols = rows // 2, rows // 8, kvw // 2
    d = lax.axis_index("dp")
    core, xb, yb = lax.rem(d, 2), lax.rem(d // 2, 2), d // 4
    sib = d + 1 - 2 * core
    xn = d + 2 - 4 * xb
    yn = d + 4 - 8 * yb
    dg = xn + 4 - 8 * yb
    blocks = (dg, xn, yn, d)

    def sibling_of(block):
        return block + 1 - 2 * core

    def columns(block, at=0, size=None):
        size = rows if size is None else size
        return pl.ds(pl.multiple_of(block * rows + at, size), size)

    barrier = pltpu.get_barrier_semaphore()
    m = lax.axis_index("mp")
    partners = [{"dp": sib}]
    partners += [{"mp": m + bit - 2 * bit * lax.rem(m // bit, 2)} for bit in zs]
    partners += [{"dp": xn}, {"dp": yn}]
    for to in partners:
        pl.semaphore_signal(barrier, inc=1, device_id=to, device_id_type=pl.DeviceIdType.MESH)

    locals_ = []

    def fetch(src, dst):
        copy = pltpu.make_async_copy(src, dst, local.at[len(locals_)])
        locals_.append(copy)
        copy.start()
        return copy

    small = [fetch(docs, lengths), fetch(freq, freqs), fetch(cot, cots)]
    own_hid = [fetch(hid.at[:, columns(block)], hh.at[i, pl.ds(0, tokens)]) for i, block in enumerate(blocks)]
    own_w = fetch(w, wv)
    own_state = fetch(state, states)
    pl.semaphore_wait(barrier, len(partners))

    copies = {}

    def begin(name, src, dst, to):
        place = len(copies)
        copies[name] = pltpu.make_async_remote_copy(
            src_ref=src,
            dst_ref=dst,
            send_sem=send.at[place],
            recv_sem=recv.at[place],
            device_id={"dp": to},
            device_id_type=pl.DeviceIdType.MESH,
        )
        copies[name].start()

    first, second = pl.ds(0, half), pl.ds(half, half)
    begin("own_x", w.at[first], wall.at[d, first], xn)
    begin("own_y", w.at[second], wall.at[d, second], yn)
    for i, block in enumerate(blocks):
        begin(("hid", i), hid.at[:, columns(sibling_of(block))], hh.at[i, pl.ds(tokens, tokens)], sib)
    begin("own_sib", w, wall.at[d], sib)

    for copy in small:
        copy.wait()
    slab = LEN // 4
    for s in range(tokens // LEN):
        start, starts = jnp.int32(0), []
        for k in range(lengths.shape[1]):
            starts.append(start)
            start = start + lengths[s, k]

        @pl.loop(0, LEN // slab)
        def _(t, s=s, starts=starts):
            place = t * slab + lax.broadcasted_iota(jnp.int32, (slab, HD), 0)
            doc_start = jnp.zeros_like(place)
            for start in starts:
                doc_start = jnp.maximum(doc_start, jnp.where(start <= place, start, 0))
            angle = (place - doc_start).astype(f32) * freqs[...]
            cos_part = jnp.cos(angle)
            sin_part = jnp.sin(angle)
            lane = lax.broadcasted_iota(jnp.int32, (slab, HD), 1)
            sin_part = jnp.where(lane < HD // 2, sin_part, -sin_part)
            at = pl.ds(pl.multiple_of(s * LEN + t * slab, slab), slab)
            for h in range(kvw // HD):
                head = pl.ds(h * HD, HD)
                value = cots[at, head].astype(f32)
                kga[at, head] = (value * cos_part + pltpu.roll(value, HD // 2, 1) * sin_part).astype(bf16)

    mine = pl.ds(0, tokens)
    begin("kg", kga.at[mine], kga.at[pl.ds(tokens, tokens)], sib)
    for copy in own_hid:
        copy.wait()
    own_w.wait()
    own_state.wait()

    def multiply(weights, block, at=0, size=rows, tile=half):
        tile = min(tile, size)

        @pl.loop(0, size // tile)
        def _(t):
            ig[:, columns(block, at + t * tile, tile)] = lax.dot_general(
                kga[mine, :], weights[pl.ds(pl.multiple_of(at + t * tile, tile), tile), :], (((1,), (1,)), ((), ())), preferred_element_type=f32
            ).astype(bf16)

    copies["kg"].wait_recv()
    for i in range(4):
        copies["hid", i].wait_recv()

        @pl.loop(0, 2)
        def _(t, i=i):
            at = pl.ds(pl.multiple_of(t * half, half), half)
            total = lax.dot_general(hh[i, :, at], kga[...], (((0,), (0,)), ((), ())), preferred_element_type=f32)
            if i == 0:
                s1x[0, at, :] = total[:, :cols].astype(bf16)
                s1y[0, at, :] = total[:, cols:].astype(bf16)
            if i == 1:
                s1x[1, at, :] = total[:, :cols].astype(bf16)
                part[0, at, :] = total[:, cols:]
            if i == 2:
                s1y[1, at, :] = total[:, cols:].astype(bf16)
                part[1, at, :] = total[:, :cols]
            if i == 3:
                part[2, at, :] = total[:, :cols]
                part[3, at, :] = total[:, cols:]

        if i == 0:
            begin(("rs1_x", 0), s1x.at[0], r1x.at[0], xn)
            begin(("rs1_y", 0), s1y.at[0], r1y.at[0], yn)
        if i == 1:
            begin(("rs1_x", 1), s1x.at[1], r1x.at[1], xn)
        if i == 2:
            begin(("rs1_y", 1), s1y.at[1], r1y.at[1], yn)

    multiply(wv, d)
    copies["own_sib"].wait_recv()
    multiply(wall.at[sib], sib)
    copies["own_x"].wait_recv()
    begin("sib_x", wall.at[xn, first], wall.at[xn, first], sib)
    copies["own_y"].wait_recv()
    begin("sib_y", wall.at[yn, second], wall.at[yn, second], sib)
    multiply(wall.at[xn], xn, 0, half)
    multiply(wall.at[yn], yn, half, half)

    copies["rs1_x", 0].wait_recv()

    @pl.loop(0, 4)
    def _(t):
        at = pl.ds(pl.multiple_of(t * (rows // 4), rows // 4), rows // 4)
        s2y[at, :] = (part[1, at, :] + r1x[0, at, :].astype(f32)).astype(bf16)

    begin("rs2_y", s2y, r2y, yn)
    copies["rs1_y", 0].wait_recv()

    @pl.loop(0, 4)
    def _(t):
        at = pl.ds(pl.multiple_of(t * (rows // 4), rows // 4), rows // 4)
        s2x[at, :] = (part[0, at, :] + r1y[0, at, :].astype(f32)).astype(bf16)

    begin("rs2_x", s2x, r2x, xn)

    def forward(k):
        low, high = pl.ds(k * step, step), pl.ds(half + k * step, step)
        begin(("fwd_x", k), wall.at[yn, high], wall.at[yn, high], xn)
        begin(("fwd_y", k), wall.at[xn, low], wall.at[xn, low], yn)

    def late(k):
        low, high = pl.ds(k * step, step), pl.ds(half + k * step, step)
        begin(("late_x", k), wv.at[high], wall.at[d, high], xn)
        begin(("late_y", k), wv.at[low], wall.at[d, low], yn)

    def pass_forward(k):
        low, high = pl.ds(k * step, step), pl.ds(half + k * step, step)
        copies["fwd_x", k].wait_recv()
        begin(("sib_fx", k), wall.at[dg, high], wall.at[dg, high], sib)
        copies["fwd_y", k].wait_recv()
        begin(("sib_fy", k), wall.at[dg, low], wall.at[dg, low], sib)

    def pass_late(k):
        low, high = pl.ds(k * step, step), pl.ds(half + k * step, step)
        copies["late_x", k].wait_recv()
        begin(("sib_lx", k), wall.at[xn, high], wall.at[xn, high], sib)
        copies["late_y", k].wait_recv()
        begin(("sib_ly", k), wall.at[yn, low], wall.at[yn, low], sib)

    for k in range(3):
        forward(k)
    copies["sib_x"].wait_recv()
    copies["sib_y"].wait_recv()
    multiply(wall.at[sibling_of(xn)], sibling_of(xn), 0, half)
    multiply(wall.at[sibling_of(yn)], sibling_of(yn), half, half)

    copies["rs1_x", 1].wait_recv()
    copies["rs1_y", 1].wait_recv()
    copies["rs2_x"].wait_recv()
    copies["rs2_y"].wait_recv()

    sums[0] = jnp.zeros_like(sums[0])
    for t in range(rows // HD):
        at = pl.ds(t * HD, HD)
        left = part[2, at, :] + r1x[1, at, :].astype(f32) + r2y[at, :].astype(f32)
        right = part[3, at, :] + r1y[1, at, :].astype(f32) + r2x[at, :].astype(f32)
        g[at, :cols] = left
        g[at, cols:] = right
        squared = left * left + right * right
        lanes = squared[:, :HD]
        for k in range(1, cols // HD):
            lanes += squared[:, k * HD : (k + 1) * HD]
        squares[at, :] = jnp.sum(lanes, axis=1, keepdims=True)
        square_rows[pl.ds(t, 1), :] = jnp.sum(lanes.T, axis=0, keepdims=True)
        sums[0] += jnp.sum(lanes.reshape(HD // 8, 8, HD), axis=0)

    def sum_begin(stage):
        copy = pltpu.make_async_remote_copy(
            src_ref=sums.at[stage],
            dst_ref=got.at[stage],
            send_sem=sum_send.at[stage],
            recv_sem=sum_recv.at[stage],
            device_id=partners[stage],
            device_id_type=pl.DeviceIdType.MESH,
        )
        copies["sum", stage] = copy
        copy.start()

    def sum_end(stage):
        copies["sum", stage].wait_recv()
        sums[stage + 1] = sums[stage] + got[stage]

    last = len(partners) - 1
    for stage in range(last - 1):
        sum_begin(stage)
        if stage == 0:
            pass_forward(0)
        sum_end(stage)
    sum_begin(last - 1)
    forward(3)
    late(0)
    pass_forward(1)
    sum_end(last - 1)
    sum_begin(last)
    for k in range(1, 4):
        late(k)
    multiply(wall.at[dg], dg, 0, 2 * step)
    multiply(wall.at[dg], dg, half, 2 * step)
    sum_end(last)
    total = jnp.sum(jnp.sum(sums[last + 1], axis=0, keepdims=True), axis=1, keepdims=True)
    clip = jnp.minimum(1.0, 1.0 / jnp.sqrt(total + 1e-06))

    for t in range(rows // HD):
        at = pl.ds(t * HD, HD)
        state_row = states[pl.ds(t, 1), :]
        new_state[pl.ds(t, 1), :] = state_row + clip * clip * (square_rows[pl.ds(t, 1), :] / kvw)
        old = jnp.broadcast_to(state_row, (HD, HD)).T
        fresh = old + clip * clip * (squares[at, :] / kvw)
        scale = learn_rate * clip / (jnp.sqrt(fresh) + 1e-10)
        for k in range(kvw // HD):
            lanes_at = pl.ds(k * HD, HD)
            new_w[at, lanes_at] = (wv[at, lanes_at].astype(f32) - scale * g[at, lanes_at]).astype(bf16)

    pass_forward(2)
    pass_forward(3)
    multiply(wall.at[dg], dg, 2 * step, 2 * step)
    multiply(wall.at[dg], dg, half + 2 * step, 2 * step)
    for k in range(4):
        copies["sib_fx", k].wait_recv()
        copies["sib_fy", k].wait_recv()
    multiply(wall.at[sibling_of(dg)], sibling_of(dg))
    for pair in range(2):
        for k in (2 * pair, 2 * pair + 1):
            pass_late(k)
        at = 2 * pair * step
        multiply(wall.at[xn], xn, half + at, 2 * step)
        multiply(wall.at[yn], yn, at, 2 * step)
        for k in (2 * pair, 2 * pair + 1):
            copies["sib_lx", k].wait_recv()
            copies["sib_ly", k].wait_recv()
        multiply(wall.at[sibling_of(xn)], sibling_of(xn), half + at, 2 * step)
        multiply(wall.at[sibling_of(yn)], sibling_of(yn), at, 2 * step)

    for copy in copies.values():
        copy.wait_send()


def shards_cube(zs, hidden, key_weight, key_state, key_cotangent, doc_lengths):
    tokens, width = hidden.shape
    rows, kvw = key_weight.shape
    cols = kvw // 2
    bf16, f32 = jnp.bfloat16, jnp.float32
    half_dim = HD // 2
    frequency = jnp.exp(
        -(2.0 * jnp.arange(half_dim, dtype=jnp.float32) / HD) * jnp.log(jnp.float32(500000.0))
    )
    frequency = jnp.concatenate([frequency, frequency])[None, :]
    held = pl.BlockSpec(memory_space=pl.ANY)
    vmem = pl.BlockSpec(memory_space=pltpu.VMEM)
    stages = len(zs) + 3
    groups = rows // HD
    input_grad, new_weight, new_state = pl.pallas_call(
        functools.partial(exchange, zs),
        out_shape=(
            pltpu.VMEM((tokens, width), bf16),
            pltpu.VMEM((rows, kvw), bf16),
            pltpu.VMEM((groups, HD), f32),
        ),
        in_specs=[held] * 6,
        out_specs=(vmem, vmem, vmem),
        scratch_shapes=[
            pltpu.VMEM((rows, kvw), bf16),
            pltpu.VMEM((groups, HD), f32),
            pltpu.VMEM((tokens, kvw), bf16),
            pltpu.SMEM(doc_lengths.shape, jnp.int32),
            pltpu.VMEM((1, HD), f32),
            pltpu.VMEM((4, 2 * tokens, rows), bf16),
            pltpu.VMEM((2 * tokens, kvw), bf16),
            pltpu.VMEM((4, rows, cols), f32),
            pltpu.VMEM((2, rows, cols), bf16),
            pltpu.VMEM((2, rows, cols), bf16),
            pltpu.VMEM((2, rows, cols), bf16),
            pltpu.VMEM((2, rows, cols), bf16),
            pltpu.VMEM((rows, cols), bf16),
            pltpu.VMEM((rows, cols), bf16),
            pltpu.VMEM((rows, cols), bf16),
            pltpu.VMEM((rows, cols), bf16),
            pltpu.VMEM((width // rows, rows, kvw), bf16),
            pltpu.VMEM((rows, kvw), f32),
            pltpu.VMEM((rows, 1), f32),
            pltpu.VMEM((groups, HD), f32),
            pltpu.VMEM((stages + 1, 8, HD), f32),
            pltpu.VMEM((stages, 8, HD), f32),
            pltpu.SemaphoreType.DMA((LOCALS,)),
            pltpu.SemaphoreType.DMA((COPIES,)),
            pltpu.SemaphoreType.DMA((COPIES,)),
            pltpu.SemaphoreType.DMA((stages,)),
            pltpu.SemaphoreType.DMA((stages,)),
        ],
        compiler_params=pltpu.CompilerParams(
            collective_id=0, has_side_effects=True, vmem_limit_bytes=56 * 1024 * 1024
        ),
    )(hidden, key_weight, key_state.reshape(groups, HD), key_cotangent, doc_lengths, frequency)
    return input_grad, new_weight, new_state.reshape(rows)


def solution(mesh):
    mp = mesh.shape["mp"]
    zs = tuple(2**k for k in range(mp.bit_length() - 1))
    cube = mesh.shape["dp"] == 2**3 and mp == 2 ** len(zs)
    return jax.shard_map(
        functools.partial(shards_cube, zs) if cube else shards,
        mesh=mesh,
        in_specs=(
            P("dp", "mp"),
            P(("mp", "dp"), None),
            P(("mp", "dp")),
            P("dp", None),
            P("dp", None),
        ),
        out_specs=(P("dp", "mp"), P(("mp", "dp"), None), P(("mp", "dp"))),
        check_vma=False,
    )
```

```python
import functools

import jax
import jax.numpy as jnp
from jax import lax
from jax.experimental import pallas as pl
from jax.experimental.pallas import tpu as pltpu
from jax.sharding import PartitionSpec as P

HD = 128
LEN = 256


learn_rate = 0.01


def positions_of(doc_lengths):
    doc_ends = jnp.cumsum(doc_lengths, axis=1)
    doc_starts = doc_ends - doc_lengths
    places = jnp.arange(LEN, dtype=jnp.int32)
    before = doc_starts[:, None, :] <= places[None, :, None]
    doc_start = jnp.max(jnp.where(before, doc_starts[:, None, :], 0), axis=2)
    return (places[None, :] - doc_start).reshape(-1)


def rope_back(cotangent, positions):
    half_dim = HD // 2
    frequency = jnp.exp(
        -(2.0 * jnp.arange(half_dim, dtype=jnp.float32) / HD) * jnp.log(jnp.float32(500000.0))
    )
    angles = positions.astype(jnp.float32)[:, None] * frequency[None, :]
    cos_part = jnp.cos(angles)[:, None, :]
    sin_part = jnp.sin(angles)[:, None, :]
    gradients = cotangent.astype(jnp.float32).reshape(cotangent.shape[0], -1, HD)
    first_half = gradients[..., :half_dim]
    second_half = gradients[..., half_dim:]
    rotated = jnp.concatenate(
        [
            first_half * cos_part + second_half * sin_part,
            second_half * cos_part - first_half * sin_part,
        ],
        axis=-1,
    )
    return rotated.reshape(cotangent.shape[0], -1).astype(jnp.bfloat16)


def update(owned, key_weight, key_state):
    squared = owned * owned
    squares_sum = lax.psum(jnp.sum(squared), ("dp", "mp"))
    clip_factor = jnp.minimum(jnp.float32(1.0), 1.0 / jnp.sqrt(squares_sum + 1e-06))
    row_mean = jnp.mean(squared, axis=1)
    new_state = key_state + clip_factor * clip_factor * row_mean
    step_size = learn_rate * clip_factor * owned / (jnp.sqrt(new_state)[:, None] + 1e-10)
    new_weight = (key_weight.astype(jnp.float32) - step_size).astype(jnp.bfloat16)
    return new_weight, new_state


def shards(hidden, key_weight, key_state, key_cotangent, doc_lengths):
    positions = positions_of(doc_lengths)
    key_grad = rope_back(key_cotangent, positions)
    gathered = lax.dot_general(
        key_grad,
        lax.all_gather(key_weight, "dp", axis=0, tiled=True),
        (((1,), (1,)), ((), ())),
        preferred_element_type=jnp.float32,
    )
    input_grad = gathered.astype(jnp.bfloat16)
    owned = lax.psum_scatter(
        lax.dot_general(
            hidden, key_grad, (((0,), (0,)), ((), ())), preferred_element_type=jnp.float32
        ),
        "dp",
        scatter_dimension=0,
        tiled=True,
    )
    return (input_grad, *update(owned, key_weight, key_state))


COPIES = 64
LOCALS = 8


def exchange(zs, hid, w, state, cot, docs, ig, new_w, new_state, kg, tails, wv, states, cots, lengths, hh, kga, part, s1x, s1y, r1x, r1y, s2x, s2y, r2x, r2y, wall, g, squares, square_rows, sums, got, local, ready, send, recv, sum_send, sum_recv):
    f32, bf16 = jnp.float32, jnp.bfloat16
    rows, kvw = wv.shape
    tokens = cots.shape[0]
    half, step, cols = rows // 2, rows // 8, kvw // 2
    d = lax.axis_index("dp")
    core, xb, yb = lax.rem(d, 2), lax.rem(d // 2, 2), d // 4
    sib = d + 1 - 2 * core
    xn = d + 2 - 4 * xb
    yn = d + 4 - 8 * yb
    dg = xn + 4 - 8 * yb
    blocks = (dg, xn, yn, d)

    def sibling_of(block):
        return block + 1 - 2 * core

    def columns(block, at=0, size=None):
        size = rows if size is None else size
        return pl.ds(pl.multiple_of(block * rows + at, size), size)

    barrier = pltpu.get_barrier_semaphore()
    m = lax.axis_index("mp")
    partners = [{"dp": sib}]
    partners += [{"mp": m + bit - 2 * bit * lax.rem(m // bit, 2)} for bit in zs]
    partners += [{"dp": xn}, {"dp": yn}]
    late_half = [core] + [lax.rem(m // bit, 2) for bit in zs]

    def signal(semaphore, to):
        pl.semaphore_signal(semaphore, inc=1, device_id=to, device_id_type=pl.DeviceIdType.MESH)

    for to in partners[-2:]:
        signal(barrier, to)
    for j, upper in enumerate(late_half):

        @pl.when(upper == 0)
        def _(j=j):
            signal(barrier, partners[j])

    def greeted(j):
        @pl.when(late_half[j] == 0)
        def _():
            pl.semaphore_wait(ready.at[j], 1)

    locals_ = []

    def fetch(src, dst):
        copy = pltpu.make_async_copy(src, dst, local.at[len(locals_)])
        locals_.append(copy)
        copy.start()
        return copy

    small = [fetch(docs, lengths), fetch(cot, cots)]
    own_hid = [fetch(hid.at[:, columns(block)], hh.at[i, pl.ds(0, tokens)]) for i, block in enumerate(blocks)]
    own_w = fetch(w, wv)
    own_state = fetch(state, states)
    pl.semaphore_wait(barrier, 2 + sum(late_half))

    copies = {}

    def begin(name, src, dst, to):
        place = len(copies)
        copies[name] = pltpu.make_async_remote_copy(
            src_ref=src,
            dst_ref=dst,
            send_sem=send.at[place],
            recv_sem=recv.at[place],
            device_id={"dp": to},
            device_id_type=pl.DeviceIdType.MESH,
        )
        copies[name].start()

    first, second = pl.ds(0, half), pl.ds(half, half)
    begin("own_x", w.at[first], wall.at[d, first], xn)
    begin("own_y", w.at[second], wall.at[d, second], yn)
    for j, upper in enumerate(late_half):

        @pl.when(upper == 1)
        def _(j=j):
            signal(ready.at[j], partners[j])

    greeted(0)
    for i, block in enumerate(blocks):
        begin(("hid", i), hid.at[:, columns(sibling_of(block))], hh.at[i, pl.ds(tokens, tokens)], sib)
    begin("own_sib", w, wall.at[d], sib)

    for copy in small:
        copy.wait()
    slab = LEN // 4
    pair = lax.rem(lax.broadcasted_iota(jnp.int32, (1, HD), 1), HD // 2).astype(f32)
    frequency = jnp.exp(-(2.0 * pair / HD) * jnp.log(jnp.float32(500000.0)))
    for s in range(tokens // LEN):
        start, starts = jnp.int32(0), []
        for k in range(lengths.shape[1]):
            starts.append(start)
            start = start + lengths[s, k]

        @pl.loop(0, LEN // slab)
        def _(t, s=s, starts=starts):
            place = t * slab + lax.broadcasted_iota(jnp.int32, (slab, HD), 0)
            doc_start = jnp.zeros_like(place)
            for start in starts:
                doc_start = jnp.maximum(doc_start, jnp.where(start <= place, start, 0))
            angle = (place - doc_start).astype(f32) * frequency
            cos_part = jnp.cos(angle)
            sin_part = jnp.sin(angle)
            lane = lax.broadcasted_iota(jnp.int32, (slab, HD), 1)
            sin_part = jnp.where(lane < HD // 2, sin_part, -sin_part)
            at = pl.ds(pl.multiple_of(s * LEN + t * slab, slab), slab)
            for h in range(kvw // HD):
                head = pl.ds(h * HD, HD)
                value = cots[at, head].astype(f32)
                turned = (value * cos_part + pltpu.roll(value, HD // 2, 1) * sin_part).astype(bf16)
                kga[at, head] = turned
                kg[at, head] = turned

    mine = pl.ds(0, tokens)
    begin("kg", kga.at[mine], kga.at[pl.ds(tokens, tokens)], sib)
    for copy in own_hid:
        copy.wait()
    own_w.wait()
    own_state.wait()

    def multiply(weights, block, at=0, size=rows, tile=half):
        tile = min(tile, size)

        @pl.loop(0, size // tile)
        def _(t):
            ig[:, columns(block, at + t * tile, tile)] = lax.dot_general(
                kga[mine, :], weights[pl.ds(pl.multiple_of(at + t * tile, tile), tile), :], (((1,), (1,)), ((), ())), preferred_element_type=f32
            ).astype(bf16)

    copies["kg"].wait_recv()
    for i in range(4):
        copies["hid", i].wait_recv()

        @pl.loop(0, 2)
        def _(t, i=i):
            at = pl.ds(pl.multiple_of(t * half, half), half)
            total = lax.dot_general(hh[i, :, at], kga[...], (((0,), (0,)), ((), ())), preferred_element_type=f32)
            if i == 0:
                s1x[0, at, :] = total[:, :cols].astype(bf16)
                s1y[0, at, :] = total[:, cols:].astype(bf16)
            if i == 1:
                s1x[1, at, :] = total[:, :cols].astype(bf16)
                part[0, at, :] = total[:, cols:]
            if i == 2:
                s1y[1, at, :] = total[:, cols:].astype(bf16)
                part[1, at, :] = total[:, :cols]
            if i == 3:
                part[2, at, :] = total[:, :cols]
                part[3, at, :] = total[:, cols:]

        if i == 0:
            begin(("rs1_x", 0), s1x.at[0], r1x.at[0], xn)
            begin(("rs1_y", 0), s1y.at[0], r1y.at[0], yn)
        if i == 1:
            begin(("rs1_x", 1), s1x.at[1], r1x.at[1], xn)
        if i == 2:
            begin(("rs1_y", 1), s1y.at[1], r1y.at[1], yn)

    multiply(wv, d)
    copies["own_sib"].wait_recv()
    multiply(wall.at[sib], sib)
    copies["own_x"].wait_recv()
    begin("sib_x", wall.at[xn, first], wall.at[xn, first], sib)
    copies["own_y"].wait_recv()
    begin("sib_y", wall.at[yn, second], wall.at[yn, second], sib)
    multiply(wall.at[xn], xn, 0, half)
    multiply(wall.at[yn], yn, half, half)

    copies["rs1_x", 0].wait_recv()

    @pl.loop(0, 4)
    def _(t):
        at = pl.ds(pl.multiple_of(t * (rows // 4), rows // 4), rows // 4)
        s2y[at, :] = (part[1, at, :] + r1x[0, at, :].astype(f32)).astype(bf16)

    begin("rs2_y", s2y, r2y, yn)
    copies["rs1_y", 0].wait_recv()

    @pl.loop(0, 4)
    def _(t):
        at = pl.ds(pl.multiple_of(t * (rows // 4), rows // 4), rows // 4)
        s2x[at, :] = (part[0, at, :] + r1y[0, at, :].astype(f32)).astype(bf16)

    begin("rs2_x", s2x, r2x, xn)

    def forward(k):
        low, high = pl.ds(k * step, step), pl.ds(half + k * step, step)
        begin(("fwd_x", k), wall.at[yn, high], wall.at[yn, high], xn)
        begin(("fwd_y", k), wall.at[xn, low], wall.at[xn, low], yn)

    def late(k):
        low, high = pl.ds(k * step, step), pl.ds(half + k * step, step)
        to_x, to_y = wall.at[d, high], wall.at[d, low]
        if k >= 2:
            to_x, to_y = (tails.at[i, pl.ds((k - 2) * step, step)] for i in range(2))
        begin(("late_x", k), wv.at[high], to_x, xn)
        begin(("late_y", k), wv.at[low], to_y, yn)

    def pass_forward(k):
        low, high = pl.ds(k * step, step), pl.ds(half + k * step, step)
        copies["fwd_x", k].wait_recv()
        begin(("sib_fx", k), wall.at[dg, high], wall.at[dg, high], sib)
        copies["fwd_y", k].wait_recv()
        begin(("sib_fy", k), wall.at[dg, low], wall.at[dg, low], sib)

    def pass_late(k):
        low, high = pl.ds(k * step, step), pl.ds(half + k * step, step)
        at = pl.ds((k - 2) * step, step)
        copies["late_x", k].wait_recv()
        if k < 2:
            begin(("sib_lx", k), wall.at[xn, high], wall.at[xn, high], sib)
        else:
            begin(("sib_lx", k), tails.at[0, at], tails.at[2, at], sib)
        copies["late_y", k].wait_recv()
        if k < 2:
            begin(("sib_ly", k), wall.at[yn, low], wall.at[yn, low], sib)
        else:
            begin(("sib_ly", k), tails.at[1, at], tails.at[3, at], sib)

    for k in range(4):
        forward(k)
    copies["sib_x"].wait_recv()
    copies["sib_y"].wait_recv()
    multiply(wall.at[sibling_of(xn)], sibling_of(xn), 0, half)
    multiply(wall.at[sibling_of(yn)], sibling_of(yn), half, half)

    copies["rs1_x", 1].wait_recv()
    copies["rs1_y", 1].wait_recv()
    copies["rs2_x"].wait_recv()
    copies["rs2_y"].wait_recv()

    sums[0] = jnp.zeros_like(sums[0])
    for t in range(rows // HD):
        at = pl.ds(t * HD, HD)
        left = part[2, at, :] + r1x[1, at, :].astype(f32) + r2y[at, :].astype(f32)
        right = part[3, at, :] + r1y[1, at, :].astype(f32) + r2x[at, :].astype(f32)
        g[at, :cols] = left
        g[at, cols:] = right
        squared = left * left + right * right
        lanes = squared[:, :HD]
        for k in range(1, cols // HD):
            lanes += squared[:, k * HD : (k + 1) * HD]
        squares[at, :] = jnp.sum(lanes, axis=1, keepdims=True)
        square_rows[pl.ds(t, 1), :] = jnp.sum(lanes.T, axis=0, keepdims=True)
        sums[0] += jnp.sum(lanes.reshape(HD // 8, 8, HD), axis=0)

    def sum_begin(stage):
        copy = pltpu.make_async_remote_copy(
            src_ref=sums.at[stage],
            dst_ref=got.at[stage],
            send_sem=sum_send.at[stage],
            recv_sem=sum_recv.at[stage],
            device_id=partners[stage],
            device_id_type=pl.DeviceIdType.MESH,
        )
        copies["sum", stage] = copy
        copy.start()

    def sum_end(stage):
        copies["sum", stage].wait_recv()
        sums[stage + 1] = sums[stage] + got[stage]

    last = len(partners) - 1
    for stage in range(last - 1):
        if stage:
            greeted(stage)
        sum_begin(stage)
        if stage == 0:
            pass_forward(0)
        sum_end(stage)
    sum_begin(last - 1)
    late(0)
    late(1)
    pass_forward(1)
    sum_end(last - 1)
    sum_begin(last)
    for k in range(2, 4):
        late(k)
    multiply(wall.at[dg], dg, 0, 2 * step)
    multiply(wall.at[dg], dg, half, 2 * step)
    sum_end(last)
    total = jnp.sum(jnp.sum(sums[last + 1], axis=0, keepdims=True), axis=1, keepdims=True)
    clip = jnp.minimum(1.0, 1.0 / jnp.sqrt(total + 1e-06))

    for t in range(rows // HD):
        at = pl.ds(t * HD, HD)
        state_row = states[pl.ds(t, 1), :]
        new_state[pl.ds(t, 1), :] = state_row + clip * clip * (square_rows[pl.ds(t, 1), :] / kvw)
        old = jnp.broadcast_to(state_row, (HD, HD)).T
        fresh = old + clip * clip * (squares[at, :] / kvw)
        scale = learn_rate * clip / (jnp.sqrt(fresh) + 1e-10)
        for k in range(kvw // HD):
            lanes_at = pl.ds(k * HD, HD)
            new_w[at, lanes_at] = (wv[at, lanes_at].astype(f32) - scale * g[at, lanes_at]).astype(bf16)

    pass_forward(2)
    pass_forward(3)
    multiply(wall.at[dg], dg, 2 * step, 2 * step)
    multiply(wall.at[dg], dg, half + 2 * step, 2 * step)
    for k in range(4):
        copies["sib_fx", k].wait_recv()
        copies["sib_fy", k].wait_recv()
    multiply(wall.at[sibling_of(dg)], sibling_of(dg))
    for k in range(2):
        pass_late(k)
    multiply(wall.at[xn], xn, half, 2 * step)
    multiply(wall.at[yn], yn, 0, 2 * step)
    for k in range(2):
        copies["sib_lx", k].wait_recv()
        copies["sib_ly", k].wait_recv()
    multiply(wall.at[sibling_of(xn)], sibling_of(xn), half, 2 * step)
    multiply(wall.at[sibling_of(yn)], sibling_of(yn), 0, 2 * step)
    for k in range(2, 4):
        pass_late(k)
    for k in range(2, 4):
        copies["sib_lx", k].wait_recv()
        copies["sib_ly", k].wait_recv()

    for copy in copies.values():
        copy.wait_send()


def finish(ig_part, kg, tails, w_part, state_part, ig, new_w, new_state, last, sems):
    rows = w_part.shape[0]
    half, tail = rows // 2, tails.shape[1]
    d = lax.axis_index("dp")
    core, xb, yb = lax.rem(d, 2), lax.rem(d // 2, 2), d // 4
    xn = d + 2 - 4 * xb
    yn = d + 4 - 8 * yb
    dg = xn + 4 - 8 * yb
    flip = 1 - 2 * core
    copies = []

    def put(src, dst):
        copy = pltpu.make_async_copy(src, dst, sems.at[len(copies)])
        copies.append(copy)
        copy.start()

    def ready(block, at, size):
        where = pl.ds(pl.multiple_of(block * rows + at, HD), size)
        put(ig_part.at[:, where], ig.at[:, where])

    for block in (d, dg):
        for owner in (block, block + flip):
            ready(owner, 0, rows)
    for owner in (xn, xn + flip):
        ready(owner, 0, rows - tail)
    for owner in (yn, yn + flip):
        ready(owner, 0, half - tail)
        ready(owner, half, half)
    put(w_part, new_w)
    put(state_part, new_state)
    for i, owner in enumerate((xn, yn, xn + flip, yn + flip)):
        last[i] = lax.dot_general(
            kg[...], tails[i], (((1,), (1,)), ((), ())), preferred_element_type=jnp.float32
        ).astype(jnp.bfloat16)
        at = (half if i % 2 else rows) - tail
        put(last.at[i], ig.at[:, pl.ds(pl.multiple_of(owner * rows + at, HD), tail)])
    for copy in copies:
        copy.wait()


def shards_cube(zs, hidden, key_weight, key_state, key_cotangent, doc_lengths):
    tokens, width = hidden.shape
    rows, kvw = key_weight.shape
    cols = kvw // 2
    bf16, f32 = jnp.bfloat16, jnp.float32
    held = pl.BlockSpec(memory_space=pl.ANY)
    vmem = pl.BlockSpec(memory_space=pltpu.VMEM)
    stages = len(zs) + 3
    groups = rows // HD
    tail = rows // 4
    *parts, kg, tails = pl.pallas_call(
        functools.partial(exchange, zs),
        out_shape=(
            pltpu.VMEM((tokens, width), bf16),
            pltpu.VMEM((rows, kvw), bf16),
            pltpu.VMEM((groups, HD), f32),
            pltpu.VMEM((tokens, kvw), bf16),
            pltpu.VMEM((4, tail, kvw), bf16),
        ),
        in_specs=[held] * 5,
        out_specs=(vmem,) * 5,
        scratch_shapes=[
            pltpu.VMEM((rows, kvw), bf16),
            pltpu.VMEM((groups, HD), f32),
            pltpu.VMEM((tokens, kvw), bf16),
            pltpu.SMEM(doc_lengths.shape, jnp.int32),
            pltpu.VMEM((4, 2 * tokens, rows), bf16),
            pltpu.VMEM((2 * tokens, kvw), bf16),
            pltpu.VMEM((4, rows, cols), f32),
            pltpu.VMEM((2, rows, cols), bf16),
            pltpu.VMEM((2, rows, cols), bf16),
            pltpu.VMEM((2, rows, cols), bf16),
            pltpu.VMEM((2, rows, cols), bf16),
            pltpu.VMEM((rows, cols), bf16),
            pltpu.VMEM((rows, cols), bf16),
            pltpu.VMEM((rows, cols), bf16),
            pltpu.VMEM((rows, cols), bf16),
            pltpu.VMEM((width // rows, rows, kvw), bf16),
            pltpu.VMEM((rows, kvw), f32),
            pltpu.VMEM((rows, 1), f32),
            pltpu.VMEM((groups, HD), f32),
            pltpu.VMEM((stages + 1, 8, HD), f32),
            pltpu.VMEM((stages, 8, HD), f32),
            pltpu.SemaphoreType.DMA((LOCALS,)),
            pltpu.SemaphoreType.REGULAR((1 + len(zs),)),
            pltpu.SemaphoreType.DMA((COPIES,)),
            pltpu.SemaphoreType.DMA((COPIES,)),
            pltpu.SemaphoreType.DMA((stages,)),
            pltpu.SemaphoreType.DMA((stages,)),
        ],
        compiler_params=pltpu.CompilerParams(
            collective_id=0, has_side_effects=True, vmem_limit_bytes=56 * 1024 * 1024
        ),
    )(hidden, key_weight, key_state.reshape(groups, HD), key_cotangent, doc_lengths)
    input_grad, new_weight, new_state = pl.pallas_call(
        finish,
        out_shape=(
            jax.ShapeDtypeStruct((tokens, width), bf16),
            jax.ShapeDtypeStruct((rows, kvw), bf16),
            jax.ShapeDtypeStruct((groups, HD), f32),
        ),
        in_specs=[held, vmem, vmem, held, held],
        out_specs=(held,) * 3,
        scratch_shapes=[pltpu.VMEM((4, tokens, tail), bf16), pltpu.SemaphoreType.DMA((16,))],
        compiler_params=pltpu.CompilerParams(vmem_limit_bytes=4 * 1024 * 1024),
    )(parts[0], kg, tails, *parts[1:])
    return input_grad, new_weight, new_state.reshape(rows)


def solution(mesh):
    mp = mesh.shape["mp"]
    zs = tuple(2**k for k in range(mp.bit_length() - 1))
    cube = mesh.shape["dp"] == 2**3 and mp == 2 ** len(zs)
    return jax.shard_map(
        functools.partial(shards_cube, zs) if cube else shards,
        mesh=mesh,
        in_specs=(
            P("dp", "mp"),
            P(("mp", "dp"), None),
            P(("mp", "dp")),
            P("dp", None),
            P("dp", None),
        ),
        out_specs=(P("dp", "mp"), P(("mp", "dp"), None), P(("mp", "dp"))),
        check_vma=False,
    )
```

```python
import functools

import jax
import jax.numpy as jnp
from jax import lax
from jax.experimental import pallas as pl
from jax.experimental.pallas import tpu as pltpu
from jax.sharding import PartitionSpec as P

HD = 128
LEN = 256


learn_rate = 0.01


def positions_of(doc_lengths):
    doc_ends = jnp.cumsum(doc_lengths, axis=1)
    doc_starts = doc_ends - doc_lengths
    places = jnp.arange(LEN, dtype=jnp.int32)
    before = doc_starts[:, None, :] <= places[None, :, None]
    doc_start = jnp.max(jnp.where(before, doc_starts[:, None, :], 0), axis=2)
    return (places[None, :] - doc_start).reshape(-1)


def rope_back(cotangent, positions):
    half_dim = HD // 2
    frequency = jnp.exp(
        -(2.0 * jnp.arange(half_dim, dtype=jnp.float32) / HD) * jnp.log(jnp.float32(500000.0))
    )
    angles = positions.astype(jnp.float32)[:, None] * frequency[None, :]
    cos_part = jnp.cos(angles)[:, None, :]
    sin_part = jnp.sin(angles)[:, None, :]
    gradients = cotangent.astype(jnp.float32).reshape(cotangent.shape[0], -1, HD)
    first_half = gradients[..., :half_dim]
    second_half = gradients[..., half_dim:]
    rotated = jnp.concatenate(
        [
            first_half * cos_part + second_half * sin_part,
            second_half * cos_part - first_half * sin_part,
        ],
        axis=-1,
    )
    return rotated.reshape(cotangent.shape[0], -1).astype(jnp.bfloat16)


def update(owned, key_weight, key_state):
    squared = owned * owned
    squares_sum = lax.psum(jnp.sum(squared), ("dp", "mp"))
    clip_factor = jnp.minimum(jnp.float32(1.0), 1.0 / jnp.sqrt(squares_sum + 1e-06))
    row_mean = jnp.mean(squared, axis=1)
    new_state = key_state + clip_factor * clip_factor * row_mean
    step_size = learn_rate * clip_factor * owned / (jnp.sqrt(new_state)[:, None] + 1e-10)
    new_weight = (key_weight.astype(jnp.float32) - step_size).astype(jnp.bfloat16)
    return new_weight, new_state


def shards(hidden, key_weight, key_state, key_cotangent, doc_lengths):
    positions = positions_of(doc_lengths)
    key_grad = rope_back(key_cotangent, positions)
    gathered = lax.dot_general(
        key_grad,
        lax.all_gather(key_weight, "dp", axis=0, tiled=True),
        (((1,), (1,)), ((), ())),
        preferred_element_type=jnp.float32,
    )
    input_grad = gathered.astype(jnp.bfloat16)
    owned = lax.psum_scatter(
        lax.dot_general(
            hidden, key_grad, (((0,), (0,)), ((), ())), preferred_element_type=jnp.float32
        ),
        "dp",
        scatter_dimension=0,
        tiled=True,
    )
    return (input_grad, *update(owned, key_weight, key_state))


COPIES = 64
LOCALS = 8


def exchange(zs, hid, w, state, cot, docs, ig, new_w, new_state, kg, tails, wv, states, cots, lengths, hh, kga, part, s1x, s1y, r1x, r1y, s2x, s2y, r2x, r2y, wall, g, squares, square_rows, sums, got, local, ready, send, recv, sum_send, sum_recv):
    f32, bf16 = jnp.float32, jnp.bfloat16
    rows, kvw = wv.shape
    tokens = cots.shape[0]
    half, step, cols = rows // 2, rows // 8, kvw // 2
    d = lax.axis_index("dp")
    core, xb, yb = lax.rem(d, 2), lax.rem(d // 2, 2), d // 4
    sib = d + 1 - 2 * core
    xn = d + 2 - 4 * xb
    yn = d + 4 - 8 * yb
    dg = xn + 4 - 8 * yb
    blocks = (dg, xn, yn, d)

    def sibling_of(block):
        return block + 1 - 2 * core

    def columns(block, at=0, size=None):
        size = rows if size is None else size
        return pl.ds(pl.multiple_of(block * rows + at, size), size)

    barrier = pltpu.get_barrier_semaphore()
    m = lax.axis_index("mp")
    partners = [{"dp": sib}, {"dp": xn}, {"dp": yn}]
    partners += [{"mp": m + bit - 2 * bit * lax.rem(m // bit, 2)} for bit in zs]
    late_half = {0: core, **{3 + j: lax.rem(m // bit, 2) for j, bit in enumerate(zs)}}

    def signal(semaphore, to):
        pl.semaphore_signal(semaphore, inc=1, device_id=to, device_id_type=pl.DeviceIdType.MESH)

    for to in partners[1:3]:
        signal(barrier, to)
    for j, upper in late_half.items():

        @pl.when(upper == 0)
        def _(j=j):
            signal(barrier, partners[j])

    def greeted(j):
        @pl.when(late_half[j] == 0)
        def _():
            pl.semaphore_wait(ready.at[j], 1)

    locals_ = []

    def fetch(src, dst):
        copy = pltpu.make_async_copy(src, dst, local.at[len(locals_)])
        locals_.append(copy)
        copy.start()
        return copy

    small = [fetch(docs, lengths), fetch(cot, cots)]
    own_hid = [fetch(hid.at[:, columns(block)], hh.at[i, pl.ds(0, tokens)]) for i, block in enumerate(blocks)]
    own_w = fetch(w, wv)
    own_state = fetch(state, states)
    pl.semaphore_wait(barrier, 2 + sum(late_half.values()))

    copies = {}

    def begin(name, src, dst, to):
        place = len(copies)
        copies[name] = pltpu.make_async_remote_copy(
            src_ref=src,
            dst_ref=dst,
            send_sem=send.at[place],
            recv_sem=recv.at[place],
            device_id={"dp": to},
            device_id_type=pl.DeviceIdType.MESH,
        )
        copies[name].start()

    first, second = pl.ds(0, half), pl.ds(half, half)
    begin("own_x", w.at[first], wall.at[d, first], xn)
    begin("own_y", w.at[second], wall.at[d, second], yn)
    for j, upper in late_half.items():

        @pl.when(upper == 1)
        def _(j=j):
            signal(ready.at[j], partners[j])

    greeted(0)
    for i, block in enumerate(blocks):
        begin(("hid", i), hid.at[:, columns(sibling_of(block))], hh.at[i, pl.ds(tokens, tokens)], sib)
    begin("own_sib", w, wall.at[d], sib)

    for copy in small:
        copy.wait()
    slab = LEN // 4
    pair = lax.rem(lax.broadcasted_iota(jnp.int32, (1, HD), 1), HD // 2).astype(f32)
    frequency = jnp.exp(-(2.0 * pair / HD) * jnp.log(jnp.float32(500000.0)))
    for s in range(tokens // LEN):
        start, starts = jnp.int32(0), []
        for k in range(lengths.shape[1]):
            starts.append(start)
            start = start + lengths[s, k]

        @pl.loop(0, LEN // slab)
        def _(t, s=s, starts=starts):
            place = t * slab + lax.broadcasted_iota(jnp.int32, (slab, HD), 0)
            doc_start = jnp.zeros_like(place)
            for start in starts:
                doc_start = jnp.maximum(doc_start, jnp.where(start <= place, start, 0))
            angle = (place - doc_start).astype(f32) * frequency
            cos_part = jnp.cos(angle)
            sin_part = jnp.sin(angle)
            lane = lax.broadcasted_iota(jnp.int32, (slab, HD), 1)
            sin_part = jnp.where(lane < HD // 2, sin_part, -sin_part)
            at = pl.ds(pl.multiple_of(s * LEN + t * slab, slab), slab)
            for h in range(kvw // HD):
                head = pl.ds(h * HD, HD)
                value = cots[at, head].astype(f32)
                turned = (value * cos_part + pltpu.roll(value, HD // 2, 1) * sin_part).astype(bf16)
                kga[at, head] = turned
                kg[at, head] = turned

    mine = pl.ds(0, tokens)
    begin("kg", kga.at[mine], kga.at[pl.ds(tokens, tokens)], sib)
    for copy in own_hid:
        copy.wait()
    own_w.wait()
    own_state.wait()

    def multiply(weights, block, at=0, size=rows, tile=half):
        tile = min(tile, size)

        @pl.loop(0, size // tile)
        def _(t):
            ig[:, columns(block, at + t * tile, tile)] = lax.dot_general(
                kga[mine, :], weights[pl.ds(pl.multiple_of(at + t * tile, tile), tile), :], (((1,), (1,)), ((), ())), preferred_element_type=f32
            ).astype(bf16)

    copies["kg"].wait_recv()
    for i in range(4):
        copies["hid", i].wait_recv()

        @pl.loop(0, 2)
        def _(t, i=i):
            at = pl.ds(pl.multiple_of(t * half, half), half)
            total = lax.dot_general(hh[i, :, at], kga[...], (((0,), (0,)), ((), ())), preferred_element_type=f32)
            if i == 0:
                s1x[0, at, :] = total[:, :cols].astype(bf16)
                s1y[0, at, :] = total[:, cols:].astype(bf16)
            if i == 1:
                s1x[1, at, :] = total[:, :cols].astype(bf16)
                part[0, at, :] = total[:, cols:]
            if i == 2:
                s1y[1, at, :] = total[:, cols:].astype(bf16)
                part[1, at, :] = total[:, :cols]
            if i == 3:
                part[2, at, :] = total[:, :cols]
                part[3, at, :] = total[:, cols:]

        if i == 0:
            begin(("rs1_x", 0), s1x.at[0], r1x.at[0], xn)
            begin(("rs1_y", 0), s1y.at[0], r1y.at[0], yn)
        if i == 1:
            begin(("rs1_x", 1), s1x.at[1], r1x.at[1], xn)
        if i == 2:
            begin(("rs1_y", 1), s1y.at[1], r1y.at[1], yn)

    multiply(wv, d)
    copies["own_sib"].wait_recv()
    multiply(wall.at[sib], sib)
    copies["own_x"].wait_recv()
    begin("sib_x", wall.at[xn, first], wall.at[xn, first], sib)
    copies["own_y"].wait_recv()
    begin("sib_y", wall.at[yn, second], wall.at[yn, second], sib)
    multiply(wall.at[xn], xn, 0, half)
    multiply(wall.at[yn], yn, half, half)

    copies["rs1_x", 0].wait_recv()

    @pl.loop(0, 4)
    def _(t):
        at = pl.ds(pl.multiple_of(t * (rows // 4), rows // 4), rows // 4)
        s2y[at, :] = (part[1, at, :] + r1x[0, at, :].astype(f32)).astype(bf16)

    begin("rs2_y", s2y, r2y, yn)
    copies["rs1_y", 0].wait_recv()

    @pl.loop(0, 4)
    def _(t):
        at = pl.ds(pl.multiple_of(t * (rows // 4), rows // 4), rows // 4)
        s2x[at, :] = (part[0, at, :] + r1y[0, at, :].astype(f32)).astype(bf16)

    begin("rs2_x", s2x, r2x, xn)

    def forward(k):
        low, high = pl.ds(k * step, step), pl.ds(half + k * step, step)
        begin(("fwd_x", k), wall.at[yn, high], wall.at[yn, high], xn)
        begin(("fwd_y", k), wall.at[xn, low], wall.at[xn, low], yn)

    def late(k):
        low, high = pl.ds(k * step, step), pl.ds(half + k * step, step)
        to_x, to_y = wall.at[d, high], wall.at[d, low]
        if k >= 2:
            to_x, to_y = (tails.at[i, pl.ds((k - 2) * step, step)] for i in range(2))
        begin(("late_x", k), wv.at[high], to_x, xn)
        begin(("late_y", k), wv.at[low], to_y, yn)

    def pass_forward(k):
        low, high = pl.ds(k * step, step), pl.ds(half + k * step, step)
        copies["fwd_x", k].wait_recv()
        begin(("sib_fx", k), wall.at[dg, high], wall.at[dg, high], sib)
        copies["fwd_y", k].wait_recv()
        begin(("sib_fy", k), wall.at[dg, low], wall.at[dg, low], sib)

    def pass_late(k):
        low, high = pl.ds(k * step, step), pl.ds(half + k * step, step)
        at = pl.ds((k - 2) * step, step)
        copies["late_x", k].wait_recv()
        if k < 2:
            begin(("sib_lx", k), wall.at[xn, high], wall.at[xn, high], sib)
        else:
            begin(("sib_lx", k), tails.at[0, at], tails.at[2, at], sib)
        copies["late_y", k].wait_recv()
        if k < 2:
            begin(("sib_ly", k), wall.at[yn, low], wall.at[yn, low], sib)
        else:
            begin(("sib_ly", k), tails.at[1, at], tails.at[3, at], sib)

    for k in range(2):
        forward(k)
    copies["sib_x"].wait_recv()
    copies["sib_y"].wait_recv()
    multiply(wall.at[sibling_of(xn)], sibling_of(xn), 0, half)
    multiply(wall.at[sibling_of(yn)], sibling_of(yn), half, half)

    copies["rs1_x", 1].wait_recv()
    copies["rs1_y", 1].wait_recv()
    copies["rs2_x"].wait_recv()
    copies["rs2_y"].wait_recv()

    sums[0] = jnp.zeros_like(sums[0])
    for t in range(rows // HD):
        at = pl.ds(t * HD, HD)
        left = part[2, at, :] + r1x[1, at, :].astype(f32) + r2y[at, :].astype(f32)
        right = part[3, at, :] + r1y[1, at, :].astype(f32) + r2x[at, :].astype(f32)
        g[at, :cols] = left
        g[at, cols:] = right
        squared = left * left + right * right
        lanes = squared[:, :HD]
        for k in range(1, cols // HD):
            lanes += squared[:, k * HD : (k + 1) * HD]
        squares[at, :] = jnp.sum(lanes, axis=1, keepdims=True)
        square_rows[pl.ds(t, 1), :] = jnp.sum(lanes.T, axis=0, keepdims=True)
        sums[0] += jnp.sum(lanes.reshape(HD // 8, 8, HD), axis=0)

    def sum_begin(stage):
        copy = pltpu.make_async_remote_copy(
            src_ref=sums.at[stage],
            dst_ref=got.at[stage],
            send_sem=sum_send.at[stage],
            recv_sem=sum_recv.at[stage],
            device_id=partners[stage],
            device_id_type=pl.DeviceIdType.MESH,
        )
        copies["sum", stage] = copy
        copy.start()

    def sum_end(stage):
        copies["sum", stage].wait_recv()
        sums[stage + 1] = sums[stage] + got[stage]

    def quarters(block, at):
        multiply(wall.at[block], block, at, 2 * step)
        multiply(wall.at[block], block, half + at, 2 * step)

    def from_sibling(names):
        for name in names:
            copies[name].wait_recv()

    sum_begin(0)
    pass_forward(0)
    sum_end(0)
    sum_begin(1)
    forward(2)
    pass_forward(1)
    sum_end(1)
    sum_begin(2)
    forward(3)
    for k in range(4):
        late(k)
    quarters(dg, 0)
    from_sibling([("sib_fx", 0), ("sib_fx", 1), ("sib_fy", 0), ("sib_fy", 1)])
    quarters(sibling_of(dg), 0)
    sum_end(2)
    last = len(partners) - 1
    for stage in range(3, last + 1):
        greeted(stage)
        sum_begin(stage)
        if stage == 3:
            pass_forward(2)
        if stage == 4:
            pass_forward(3)
        sum_end(stage)
    total = jnp.sum(jnp.sum(sums[last + 1], axis=0, keepdims=True), axis=1, keepdims=True)
    clip = jnp.minimum(1.0, 1.0 / jnp.sqrt(total + 1e-06))

    for t in range(rows // HD):
        at = pl.ds(t * HD, HD)
        state_row = states[pl.ds(t, 1), :]
        new_state[pl.ds(t, 1), :] = state_row + clip * clip * (square_rows[pl.ds(t, 1), :] / kvw)
        old = jnp.broadcast_to(state_row, (HD, HD)).T
        fresh = old + clip * clip * (squares[at, :] / kvw)
        scale = learn_rate * clip / (jnp.sqrt(fresh) + 1e-10)
        for k in range(kvw // HD):
            lanes_at = pl.ds(k * HD, HD)
            new_w[at, lanes_at] = (wv[at, lanes_at].astype(f32) - scale * g[at, lanes_at]).astype(bf16)

    if last < 3:
        pass_forward(2)
    if last < 4:
        pass_forward(3)
    quarters(dg, 2 * step)
    from_sibling([("sib_fx", 2), ("sib_fx", 3), ("sib_fy", 2), ("sib_fy", 3)])
    quarters(sibling_of(dg), 2 * step)
    for k in range(2):
        pass_late(k)
    multiply(wall.at[xn], xn, half, 2 * step)
    multiply(wall.at[yn], yn, 0, 2 * step)
    for k in range(2):
        copies["sib_lx", k].wait_recv()
        copies["sib_ly", k].wait_recv()
    multiply(wall.at[sibling_of(xn)], sibling_of(xn), half, 2 * step)
    multiply(wall.at[sibling_of(yn)], sibling_of(yn), 0, 2 * step)
    for k in range(2, 4):
        pass_late(k)
    for k in range(2, 4):
        copies["sib_lx", k].wait_recv()
        copies["sib_ly", k].wait_recv()

    for copy in copies.values():
        copy.wait_send()


def finish(ig_part, kg, tails, w_part, state_part, ig, new_w, new_state, last, sems):
    rows = w_part.shape[0]
    half, tail = rows // 2, tails.shape[1]
    d = lax.axis_index("dp")
    core, xb, yb = lax.rem(d, 2), lax.rem(d // 2, 2), d // 4
    xn = d + 2 - 4 * xb
    yn = d + 4 - 8 * yb
    dg = xn + 4 - 8 * yb
    flip = 1 - 2 * core
    copies = []

    def put(src, dst):
        copy = pltpu.make_async_copy(src, dst, sems.at[len(copies)])
        copies.append(copy)
        copy.start()

    def ready(block, at, size):
        where = pl.ds(pl.multiple_of(block * rows + at, HD), size)
        put(ig_part.at[:, where], ig.at[:, where])

    for block in (d, dg):
        for owner in (block, block + flip):
            ready(owner, 0, rows)
    for owner in (xn, xn + flip):
        ready(owner, 0, rows - tail)
    for owner in (yn, yn + flip):
        ready(owner, 0, half - tail)
        ready(owner, half, half)
    put(w_part, new_w)
    put(state_part, new_state)
    for i, owner in enumerate((xn, yn, xn + flip, yn + flip)):
        last[i] = lax.dot_general(
            kg[...], tails[i], (((1,), (1,)), ((), ())), preferred_element_type=jnp.float32
        ).astype(jnp.bfloat16)
        at = (half if i % 2 else rows) - tail
        put(last.at[i], ig.at[:, pl.ds(pl.multiple_of(owner * rows + at, HD), tail)])
    for copy in copies:
        copy.wait()


def shards_cube(zs, hidden, key_weight, key_state, key_cotangent, doc_lengths):
    tokens, width = hidden.shape
    rows, kvw = key_weight.shape
    cols = kvw // 2
    bf16, f32 = jnp.bfloat16, jnp.float32
    held = pl.BlockSpec(memory_space=pl.ANY)
    vmem = pl.BlockSpec(memory_space=pltpu.VMEM)
    stages = len(zs) + 3
    groups = rows // HD
    tail = rows // 4
    *parts, kg, tails = pl.pallas_call(
        functools.partial(exchange, zs),
        out_shape=(
            pltpu.VMEM((tokens, width), bf16),
            pltpu.VMEM((rows, kvw), bf16),
            pltpu.VMEM((groups, HD), f32),
            pltpu.VMEM((tokens, kvw), bf16),
            pltpu.VMEM((4, tail, kvw), bf16),
        ),
        in_specs=[held] * 5,
        out_specs=(vmem,) * 5,
        scratch_shapes=[
            pltpu.VMEM((rows, kvw), bf16),
            pltpu.VMEM((groups, HD), f32),
            pltpu.VMEM((tokens, kvw), bf16),
            pltpu.SMEM(doc_lengths.shape, jnp.int32),
            pltpu.VMEM((4, 2 * tokens, rows), bf16),
            pltpu.VMEM((2 * tokens, kvw), bf16),
            pltpu.VMEM((4, rows, cols), f32),
            pltpu.VMEM((2, rows, cols), bf16),
            pltpu.VMEM((2, rows, cols), bf16),
            pltpu.VMEM((2, rows, cols), bf16),
            pltpu.VMEM((2, rows, cols), bf16),
            pltpu.VMEM((rows, cols), bf16),
            pltpu.VMEM((rows, cols), bf16),
            pltpu.VMEM((rows, cols), bf16),
            pltpu.VMEM((rows, cols), bf16),
            pltpu.VMEM((width // rows, rows, kvw), bf16),
            pltpu.VMEM((rows, kvw), f32),
            pltpu.VMEM((rows, 1), f32),
            pltpu.VMEM((groups, HD), f32),
            pltpu.VMEM((stages + 1, 8, HD), f32),
            pltpu.VMEM((stages, 8, HD), f32),
            pltpu.SemaphoreType.DMA((LOCALS,)),
            pltpu.SemaphoreType.REGULAR((stages,)),
            pltpu.SemaphoreType.DMA((COPIES,)),
            pltpu.SemaphoreType.DMA((COPIES,)),
            pltpu.SemaphoreType.DMA((stages,)),
            pltpu.SemaphoreType.DMA((stages,)),
        ],
        compiler_params=pltpu.CompilerParams(
            collective_id=0, has_side_effects=True, vmem_limit_bytes=56 * 1024 * 1024
        ),
    )(hidden, key_weight, key_state.reshape(groups, HD), key_cotangent, doc_lengths)
    input_grad, new_weight, new_state = pl.pallas_call(
        finish,
        out_shape=(
            jax.ShapeDtypeStruct((tokens, width), bf16),
            jax.ShapeDtypeStruct((rows, kvw), bf16),
            jax.ShapeDtypeStruct((groups, HD), f32),
        ),
        in_specs=[held, vmem, vmem, held, held],
        out_specs=(held,) * 3,
        scratch_shapes=[pltpu.VMEM((4, tokens, tail), bf16), pltpu.SemaphoreType.DMA((16,))],
        compiler_params=pltpu.CompilerParams(vmem_limit_bytes=4 * 1024 * 1024),
    )(parts[0], kg, tails, *parts[1:])
    return input_grad, new_weight, new_state.reshape(rows)


def solution(mesh):
    mp = mesh.shape["mp"]
    zs = tuple(2**k for k in range(mp.bit_length() - 1))
    cube = mesh.shape["dp"] == 2**3 and mp == 2 ** len(zs)
    return jax.shard_map(
        functools.partial(shards_cube, zs) if cube else shards,
        mesh=mesh,
        in_specs=(
            P("dp", "mp"),
            P(("mp", "dp"), None),
            P(("mp", "dp")),
            P("dp", None),
            P("dp", None),
        ),
        out_specs=(P("dp", "mp"), P(("mp", "dp"), None), P(("mp", "dp"))),
        check_vma=False,
    )
```

```python
import functools

import jax
import jax.numpy as jnp
from jax import lax
from jax.experimental import pallas as pl
from jax.experimental.pallas import tpu as pltpu
from jax.sharding import PartitionSpec as P

HD = 128
LEN = 256


learn_rate = 0.01


def positions_of(doc_lengths):
    doc_ends = jnp.cumsum(doc_lengths, axis=1)
    doc_starts = doc_ends - doc_lengths
    places = jnp.arange(LEN, dtype=jnp.int32)
    before = doc_starts[:, None, :] <= places[None, :, None]
    doc_start = jnp.max(jnp.where(before, doc_starts[:, None, :], 0), axis=2)
    return (places[None, :] - doc_start).reshape(-1)


def rope_back(cotangent, positions):
    half_dim = HD // 2
    frequency = jnp.exp(
        -(2.0 * jnp.arange(half_dim, dtype=jnp.float32) / HD) * jnp.log(jnp.float32(500000.0))
    )
    angles = positions.astype(jnp.float32)[:, None] * frequency[None, :]
    cos_part = jnp.cos(angles)[:, None, :]
    sin_part = jnp.sin(angles)[:, None, :]
    gradients = cotangent.astype(jnp.float32).reshape(cotangent.shape[0], -1, HD)
    first_half = gradients[..., :half_dim]
    second_half = gradients[..., half_dim:]
    rotated = jnp.concatenate(
        [
            first_half * cos_part + second_half * sin_part,
            second_half * cos_part - first_half * sin_part,
        ],
        axis=-1,
    )
    return rotated.reshape(cotangent.shape[0], -1).astype(jnp.bfloat16)


def update(owned, key_weight, key_state):
    squared = owned * owned
    squares_sum = lax.psum(jnp.sum(squared), ("dp", "mp"))
    clip_factor = jnp.minimum(jnp.float32(1.0), 1.0 / jnp.sqrt(squares_sum + 1e-06))
    row_mean = jnp.mean(squared, axis=1)
    new_state = key_state + clip_factor * clip_factor * row_mean
    step_size = learn_rate * clip_factor * owned / (jnp.sqrt(new_state)[:, None] + 1e-10)
    new_weight = (key_weight.astype(jnp.float32) - step_size).astype(jnp.bfloat16)
    return new_weight, new_state


def shards(hidden, key_weight, key_state, key_cotangent, doc_lengths):
    positions = positions_of(doc_lengths)
    key_grad = rope_back(key_cotangent, positions)
    gathered = lax.dot_general(
        key_grad,
        lax.all_gather(key_weight, "dp", axis=0, tiled=True),
        (((1,), (1,)), ((), ())),
        preferred_element_type=jnp.float32,
    )
    input_grad = gathered.astype(jnp.bfloat16)
    owned = lax.psum_scatter(
        lax.dot_general(
            hidden, key_grad, (((0,), (0,)), ((), ())), preferred_element_type=jnp.float32
        ),
        "dp",
        scatter_dimension=0,
        tiled=True,
    )
    return (input_grad, *update(owned, key_weight, key_state))


OWN, HID, OWN_SIB, KG, RS1, RS2, SIB_OWN, FWD, LATE, CLOSE, SIB_FWD, SIB_LATE, SIB_CLOSE, SUM, PLANE, MP = (
    0, 1, 2, 3, 4, 5, 6, 7, 9, 10, 13, 15, 16, 17, 18, 19)
EARLY, MIDDLE, LAST, SUMS = 0, 1, 2, 3
DOCS, COT, BIG, STATE = 0, 1, 2, 3


def exchange(zs, hid, w, state, cot, docs, ig, new_w, new_state, kg, tails, wv, states, cots, lengths, hh, kga, part, s1x, s1y, r1x, r1y, s2x, s2y, r2x, r2y, wall, g, squares, square_rows, sums, got, whole, local, ready, send, recv):
    f32, bf16 = jnp.float32, jnp.bfloat16
    rows, kvw = wv.shape
    tokens = cots.shape[0]
    half, step, cols = rows // 2, rows // 4, kvw // 2
    d = lax.axis_index("dp")
    core, xb, yb = lax.rem(d, 2), lax.rem(d // 2, 2), d // 4
    sib = d + 1 - 2 * core
    xn = d + 2 - 4 * xb
    yn = d + 4 - 8 * yb
    dg = xn + 4 - 8 * yb
    blocks = (dg, xn, yn, d)

    def sibling_of(block):
        return block + 1 - 2 * core

    def columns(block, at=0, size=None):
        size = rows if size is None else size
        return pl.ds(pl.multiple_of(block * rows + at, size), size)

    barrier = pltpu.get_barrier_semaphore()
    m = lax.axis_index("mp")
    partners = [{"dp": sib}]
    partners += [{"mp": m + bit - 2 * bit * lax.rem(m // bit, 2)} for bit in zs]
    waits = {0: 1 - core, **{1 + j: core * lax.rem(m // bit, 2) for j, bit in enumerate(zs)}}
    asks = {0: core, **{1 + j: core * (1 - lax.rem(m // bit, 2)) for j, bit in enumerate(zs)}}

    def signal(semaphore, to):
        pl.semaphore_signal(semaphore, inc=1, device_id=to, device_id_type=pl.DeviceIdType.MESH)

    for to in (xn, yn):
        signal(barrier, {"dp": to})
    for j, ask in asks.items():

        @pl.when(ask == 1)
        def _(j=j):
            signal(barrier, partners[j])

    def greeted(j):
        @pl.when(asks[j] == 1)
        def _():
            pl.semaphore_wait(ready.at[j], 1)

    pl.semaphore_wait(barrier, 2 + sum(waits.values()))

    def on(which, act):
        if which is None:
            act()
        else:
            pl.when(core == which)(act)

    def begin(place, sent, src, dst, to, by=None):
        copy = pltpu.make_async_remote_copy(
            src_ref=src,
            dst_ref=dst,
            send_sem=send.at[sent],
            recv_sem=recv.at[place],
            device_id=to if isinstance(to, dict) else {"dp": to},
            device_id_type=pl.DeviceIdType.MESH,
        )
        on(by, copy.start)

    def take(semaphore, like, by=None):
        on(by, pltpu.make_async_copy(like, like, semaphore).wait)

    def lines(count):
        parts = next(n for n in range(1, wall.shape[0] + 1) if count % n == 0 and count // n <= rows)
        return wall.at[pl.ds(0, parts), pl.ds(0, count // parts)]

    def arrived(place, count, by=None):
        take(recv.at[place], lines(count), by)

    first, second = pl.ds(0, half), pl.ds(half, half)
    begin(OWN, EARLY, w.at[first], wall.at[d, first], xn)
    begin(OWN, EARLY, w.at[second], wall.at[d, second], yn)
    for j, wait in waits.items():

        @pl.when(wait == 1)
        def _(j=j):
            signal(ready.at[j], partners[j])

    def fetch(place, src, dst):
        pltpu.make_async_copy(src, dst, local.at[place]).start()

    fetch(DOCS, docs, lengths)
    fetch(COT, cot, cots)
    for i, block in enumerate(blocks):
        fetch(BIG, hid.at[:, columns(block)], hh.at[i, pl.ds(0, tokens)])
    fetch(BIG, w, wv)
    fetch(STATE, state, states)
    greeted(0)
    for i, block in enumerate(blocks):
        begin(HID, EARLY, hid.at[:, columns(sibling_of(block))], hh.at[i, pl.ds(tokens, tokens)], sib)
    begin(OWN_SIB, EARLY, w, wall.at[d], sib)

    take(local.at[DOCS], lengths)
    take(local.at[COT], cots)
    slab = LEN // 4
    pair = lax.rem(lax.broadcasted_iota(jnp.int32, (1, HD), 1), HD // 2).astype(f32)
    frequency = jnp.exp(-(2.0 * pair / HD) * jnp.log(jnp.float32(500000.0)))
    for s in range(tokens // LEN):
        start, starts = jnp.int32(0), []
        for k in range(lengths.shape[1]):
            starts.append(start)
            start = start + lengths[s, k]

        @pl.loop(0, LEN // slab)
        def _(t, s=s, starts=starts):
            place = t * slab + lax.broadcasted_iota(jnp.int32, (slab, HD), 0)
            doc_start = jnp.zeros_like(place)
            for start in starts:
                doc_start = jnp.maximum(doc_start, jnp.where(start <= place, start, 0))
            angle = (place - doc_start).astype(f32) * frequency
            cos_part = jnp.cos(angle)
            sin_part = jnp.sin(angle)
            lane = lax.broadcasted_iota(jnp.int32, (slab, HD), 1)
            sin_part = jnp.where(lane < HD // 2, sin_part, -sin_part)
            at = pl.ds(pl.multiple_of(s * LEN + t * slab, slab), slab)
            for h in range(kvw // HD):
                head = pl.ds(h * HD, HD)
                value = cots[at, head].astype(f32)
                turned = (value * cos_part + pltpu.roll(value, HD // 2, 1) * sin_part).astype(bf16)
                kga[at, head] = turned
                kg[at, head] = turned

    mine = pl.ds(0, tokens)
    begin(KG, EARLY, kga.at[mine], kga.at[pl.ds(tokens, tokens)], sib)
    block_lines = tokens * rows // kvw
    take(local.at[BIG], lines(4 * block_lines + rows))
    take(local.at[STATE], states)

    def multiply(weights, block, at=0, size=rows, tile=half):
        tile = min(tile, size)

        @pl.loop(0, size // tile)
        def _(t):
            ig[:, columns(block, at + t * tile, tile)] = lax.dot_general(
                kga[mine, :], weights[pl.ds(pl.multiple_of(at + t * tile, tile), tile), :], (((1,), (1,)), ((), ())), preferred_element_type=f32
            ).astype(bf16)

    arrived(KG, tokens)
    arrived(HID, 4 * block_lines)
    for i in range(4):
        @pl.loop(0, 2)
        def _(t, i=i):
            at = pl.ds(pl.multiple_of(t * half, half), half)
            total = lax.dot_general(hh[i, :, at], kga[...], (((0,), (0,)), ((), ())), preferred_element_type=f32)
            if i == 0:
                s1x[0, at, :] = total[:, :cols].astype(bf16)
                s1y[0, at, :] = total[:, cols:].astype(bf16)
            if i == 1:
                s1x[1, at, :] = total[:, :cols].astype(bf16)
                part[0, at, :] = total[:, cols:]
            if i == 2:
                s1y[1, at, :] = total[:, cols:].astype(bf16)
                part[1, at, :] = total[:, :cols]
            if i == 3:
                part[2, at, :] = total[:, :cols]
                part[3, at, :] = total[:, cols:]

        if i == 0:
            begin(RS1, EARLY, s1x.at[0], r1x.at[0], xn)
            begin(RS1, EARLY, s1y.at[0], r1y.at[0], yn)
        if i == 1:
            begin(RS2, EARLY, s1x.at[1], r1x.at[1], xn)
        if i == 2:
            begin(RS2, EARLY, s1y.at[1], r1y.at[1], yn)

    multiply(wv, d)
    arrived(OWN_SIB, rows)
    multiply(wall.at[sib], sib)
    arrived(OWN, rows)
    begin(SIB_OWN, MIDDLE, wall.at[xn, first], wall.at[xn, first], sib)
    begin(SIB_OWN, MIDDLE, wall.at[yn, second], wall.at[yn, second], sib)
    multiply(wall.at[xn], xn, 0, half)
    multiply(wall.at[yn], yn, half, half)

    arrived(RS1, rows)

    @pl.loop(0, 4)
    def _(t):
        at = pl.ds(pl.multiple_of(t * (rows // 4), rows // 4), rows // 4)
        s2y[at, :] = (part[1, at, :] + r1x[0, at, :].astype(f32)).astype(bf16)

    begin(RS2, EARLY, s2y, r2y, yn)

    @pl.loop(0, 4)
    def _(t):
        at = pl.ds(pl.multiple_of(t * (rows // 4), rows // 4), rows // 4)
        s2x[at, :] = (part[0, at, :] + r1y[0, at, :].astype(f32)).astype(bf16)

    begin(RS2, EARLY, s2x, r2x, xn)

    def spans(k):
        return pl.ds(k * step, step), pl.ds(half + k * step, step)

    def forward(k):
        low, high = spans(k)
        begin(FWD + k, MIDDLE, wall.at[yn, high], wall.at[yn, high], xn)
        begin(FWD + k, MIDDLE, wall.at[xn, low], wall.at[xn, low], yn)

    def pass_forward(k):
        arrived(FWD + k, 2 * step)
        for span in spans(k):
            begin(SIB_FWD + k, MIDDLE, wall.at[dg, span], wall.at[dg, span], sib)

    def late():
        low, high = spans(0)
        begin(LATE, MIDDLE, wv.at[high], wall.at[d, high], xn)
        begin(LATE, MIDDLE, wv.at[low], wall.at[d, low], yn)

    def pass_late():
        low, high = spans(0)
        arrived(LATE, 2 * step)
        begin(SIB_LATE, MIDDLE, wall.at[xn, high], wall.at[xn, high], sib)
        begin(SIB_LATE, MIDDLE, wall.at[yn, low], wall.at[yn, low], sib)

    moved = step // 4
    pieces = (
        (None, 0, 0, step // 2),
        (0, 1, step // 2, step // 2 - moved),
        (1, 1, step // 2, step // 2),
        (1, 2, step - moved, moved),
    )

    def close():
        for by, place, at, size in pieces:
            source, slot = (wall.at[sib], 2) if place == 2 else (wv, 0)
            for j, base, to in ((0, rows, xn), (1, half, yn)):
                src = source.at[pl.ds(base - step + at, size)]
                begin(CLOSE + place, LAST, src, tails.at[slot + j, pl.ds(at, size)], to, by)

    def pass_close():
        for by, place, at, size in pieces:
            slot = 2 if place == 2 else 0
            arrived(CLOSE + place, 2 * size, by)
            for j in range(2):
                part_of = pl.ds(at, size)
                begin(SIB_CLOSE, LAST, tails.at[slot + j, part_of], tails.at[2 - slot + j, part_of], sib, by)

    forward(0)
    arrived(SIB_OWN, rows)
    multiply(wall.at[sibling_of(xn)], sibling_of(xn), 0, half)
    multiply(wall.at[sibling_of(yn)], sibling_of(yn), half, half)

    arrived(RS2, 2 * rows)

    sums[0] = jnp.zeros_like(sums[0])
    for t in range(rows // HD):
        at = pl.ds(t * HD, HD)
        left = part[2, at, :] + r1x[1, at, :].astype(f32) + r2y[at, :].astype(f32)
        right = part[3, at, :] + r1y[1, at, :].astype(f32) + r2x[at, :].astype(f32)
        g[at, :cols] = left
        g[at, cols:] = right
        squared = left * left + right * right
        lanes = squared[:, :HD]
        for k in range(1, cols // HD):
            lanes += squared[:, k * HD : (k + 1) * HD]
        squares[at, :] = jnp.sum(lanes, axis=1, keepdims=True)
        square_rows[pl.ds(t, 1), :] = jnp.sum(lanes.T, axis=0, keepdims=True)
        sums[0] += jnp.sum(lanes.reshape(HD // 8, 8, HD), axis=0)

    def quarters(block, at):
        multiply(wall.at[block], block, at, step)
        multiply(wall.at[block], block, half + at, step)

    last = 2 + len(zs)

    def add(into, places):
        @pl.when(core == 1)
        def _():
            if len(places) == 1:
                sums[into] = sums[into - 1] + got[places[0]]
            else:
                sums[into] = (sums[into - 1] + got[places[0]]) + (got[places[1]] + got[places[2]])

    begin(SUM, SUMS, sums.at[0], got.at[0], sib, 0)
    take(recv.at[SUM], whole, 1)
    add(1, [0])
    for j, to in enumerate((xn, yn, dg)):
        begin(PLANE, SUMS, sums.at[1], got.at[1 + j], to, 1)
    forward(1)
    late()
    close()
    pass_forward(0)
    quarters(dg, 0)
    take(recv.at[PLANE], got.at[pl.ds(1, 3)], 1)
    add(2, [1, 2, 3])
    for j in range(len(zs)):
        greeted(1 + j)
        begin(MP + j, SUMS, sums.at[2 + j], got.at[4 + j], partners[1 + j], 1)
        if j == 0:
            arrived(SIB_FWD, 2 * step)
            quarters(sibling_of(dg), 0)
        take(recv.at[MP + j], whole, 1)
        add(3 + j, [4 + j])

    @pl.when(core == 1)
    def _():
        whole[...] = sums[last]

    begin(SUM, SUMS, sums.at[last], whole, sib, 1)
    take(recv.at[SUM], whole, 0)
    total = jnp.sum(jnp.sum(whole[...], axis=0, keepdims=True), axis=1, keepdims=True)
    clip = jnp.minimum(1.0, 1.0 / jnp.sqrt(total + 1e-06))

    for t in range(rows // HD):
        at = pl.ds(t * HD, HD)
        state_row = states[pl.ds(t, 1), :]
        new_state[pl.ds(t, 1), :] = state_row + clip * clip * (square_rows[pl.ds(t, 1), :] / kvw)
        old = jnp.broadcast_to(state_row, (HD, HD)).T
        fresh = old + clip * clip * (squares[at, :] / kvw)
        scale = learn_rate * clip / (jnp.sqrt(fresh) + 1e-10)
        for k in range(kvw // HD):
            lanes_at = pl.ds(k * HD, HD)
            new_w[at, lanes_at] = (wv[at, lanes_at].astype(f32) - scale * g[at, lanes_at]).astype(bf16)

    pass_forward(1)
    quarters(dg, step)
    arrived(SIB_FWD + 1, 2 * step)
    quarters(sibling_of(dg), step)
    pass_late()
    multiply(wall.at[xn], xn, half, step)
    multiply(wall.at[yn], yn, 0, step)
    arrived(SIB_LATE, 2 * step)
    multiply(wall.at[sibling_of(xn)], sibling_of(xn), half, step)
    multiply(wall.at[sibling_of(yn)], sibling_of(yn), 0, step)
    pass_close()
    counts = [2 * sum(size for by, _, _, size in pieces if by in (None, which)) for which in range(2)]
    for which in range(2):
        arrived(SIB_CLOSE, counts[1 - which], which)
    take(send.at[EARLY], lines(tokens + 5 * rows + 4 * block_lines))
    take(send.at[MIDDLE], lines(4 * rows))
    for which in range(2):
        take(send.at[LAST], lines(2 * counts[which]), which)
    take(send.at[SUMS], whole, 0)
    take(send.at[SUMS], got.at[pl.ds(0, 4 + len(zs))], 1)


def finish(ig_part, kg, tails, w_part, state_part, ig, new_w, new_state, last, sems):
    rows = w_part.shape[0]
    half, tail = rows // 2, tails.shape[1]
    d = lax.axis_index("dp")
    core, xb, yb = lax.rem(d, 2), lax.rem(d // 2, 2), d // 4
    xn = d + 2 - 4 * xb
    yn = d + 4 - 8 * yb
    dg = xn + 4 - 8 * yb
    flip = 1 - 2 * core

    def put(src, dst, place=0):
        copy = pltpu.make_async_copy(src, dst, sems.at[place])
        copy.start()
        return copy

    def ready(block, at, size):
        where = pl.ds(pl.multiple_of(block * rows + at, HD), size)
        put(ig_part.at[:, where], ig.at[:, where])

    for block in (d, dg):
        for owner in (block, block + flip):
            ready(owner, 0, rows)
    for owner in (xn, xn + flip):
        ready(owner, 0, rows - tail)
    for owner in (yn, yn + flip):
        ready(owner, 0, half - tail)
        ready(owner, half, half)
    others = put(w_part, new_w, 1), put(state_part, new_state, 2)
    for i, owner in enumerate((xn, yn, xn + flip, yn + flip)):
        last[i] = lax.dot_general(
            kg[...], tails[i], (((1,), (1,)), ((), ())), preferred_element_type=jnp.float32
        ).astype(jnp.bfloat16)
        at = (half if i % 2 else rows) - tail
        put(last.at[i], ig.at[:, pl.ds(pl.multiple_of(owner * rows + at, HD), tail)])
    pltpu.make_async_copy(ig_part, ig, sems.at[0]).wait()
    for copy in others:
        copy.wait()


def shards_cube(zs, hidden, key_weight, key_state, key_cotangent, doc_lengths):
    tokens, width = hidden.shape
    rows, kvw = key_weight.shape
    cols = kvw // 2
    bf16, f32 = jnp.bfloat16, jnp.float32
    held = pl.BlockSpec(memory_space=pl.ANY)
    vmem = pl.BlockSpec(memory_space=pltpu.VMEM)
    stages = len(zs) + 3
    groups = rows // HD
    tail = rows // 4
    *parts, kg, tails = pl.pallas_call(
        functools.partial(exchange, zs),
        out_shape=(
            pltpu.VMEM((tokens, width), bf16),
            pltpu.VMEM((rows, kvw), bf16),
            pltpu.VMEM((groups, HD), f32),
            pltpu.VMEM((tokens, kvw), bf16),
            pltpu.VMEM((4, tail, kvw), bf16),
        ),
        in_specs=[held] * 5,
        out_specs=(vmem,) * 5,
        scratch_shapes=[
            pltpu.VMEM((rows, kvw), bf16),
            pltpu.VMEM((groups, HD), f32),
            pltpu.VMEM((tokens, kvw), bf16),
            pltpu.SMEM(doc_lengths.shape, jnp.int32),
            pltpu.VMEM((4, 2 * tokens, rows), bf16),
            pltpu.VMEM((2 * tokens, kvw), bf16),
            pltpu.VMEM((4, rows, cols), f32),
            pltpu.VMEM((2, rows, cols), bf16),
            pltpu.VMEM((2, rows, cols), bf16),
            pltpu.VMEM((2, rows, cols), bf16),
            pltpu.VMEM((2, rows, cols), bf16),
            pltpu.VMEM((rows, cols), bf16),
            pltpu.VMEM((rows, cols), bf16),
            pltpu.VMEM((rows, cols), bf16),
            pltpu.VMEM((rows, cols), bf16),
            pltpu.VMEM((width // rows, rows, kvw), bf16),
            pltpu.VMEM((rows, kvw), f32),
            pltpu.VMEM((rows, 1), f32),
            pltpu.VMEM((groups, HD), f32),
            pltpu.VMEM((stages, 8, HD), f32),
            pltpu.VMEM((stages + 1, 8, HD), f32),
            pltpu.VMEM((8, HD), f32),
            pltpu.SemaphoreType.DMA((STATE + 1,)),
            pltpu.SemaphoreType.REGULAR((1 + len(zs),)),
            pltpu.SemaphoreType.DMA((SUMS + 1,)),
            pltpu.SemaphoreType.DMA((MP + len(zs),)),
        ],
        compiler_params=pltpu.CompilerParams(
            collective_id=0, has_side_effects=True, vmem_limit_bytes=56 * 1024 * 1024
        ),
    )(hidden, key_weight, key_state.reshape(groups, HD), key_cotangent, doc_lengths)
    input_grad, new_weight, new_state = pl.pallas_call(
        finish,
        out_shape=(
            jax.ShapeDtypeStruct((tokens, width), bf16),
            jax.ShapeDtypeStruct((rows, kvw), bf16),
            jax.ShapeDtypeStruct((groups, HD), f32),
        ),
        in_specs=[held, vmem, vmem, held, held],
        out_specs=(held,) * 3,
        scratch_shapes=[pltpu.VMEM((4, tokens, tail), bf16), pltpu.SemaphoreType.DMA((3,))],
        compiler_params=pltpu.CompilerParams(vmem_limit_bytes=4 * 1024 * 1024),
    )(parts[0], kg, tails, *parts[1:])
    return input_grad, new_weight, new_state.reshape(rows)


def solution(mesh):
    mp = mesh.shape["mp"]
    zs = tuple(2**k for k in range(mp.bit_length() - 1))
    cube = mesh.shape["dp"] == 2**3 and mp == 2 ** len(zs)
    return jax.shard_map(
        functools.partial(shards_cube, zs) if cube else shards,
        mesh=mesh,
        in_specs=(
            P("dp", "mp"),
            P(("mp", "dp"), None),
            P(("mp", "dp")),
            P("dp", None),
            P("dp", None),
        ),
        out_specs=(P("dp", "mp"), P(("mp", "dp"), None), P(("mp", "dp"))),
        check_vma=False,
    )
```
